32 devices in a mesh: grp: 8 (over z, y), mem: 4 (over x, core).
Axes of the slice: x: 2, y: 2, z: 4, core: 2. Of those that a mesh axis runs over, the one named last changes fastest.
Arguments:
- client_input: bfloat16 [8, 4, 128, 896], P('grp', 'mem'), may hold values from -6 to 6
- client_gain: float32 [4, 896], P('mem'), may hold values from 0.5 to 1.5
- w_query: bfloat16 [4, 896, 896], P('mem'), may hold values from -1.5 to 1.5
- w_keyval: bfloat16 [4, 896, 256], P('mem'), may hold values from -0.5 to 0.5
- w_out: bfloat16 [4, 896, 896], P('mem'), may hold values from -0.1875 to 0.1875
- server_gain: float32 [8, 896], P('grp'), may hold values from 0.5 to 1.5
- w_gate: bfloat16 [8, 896, 4864], P('grp', None, 'mem'), may hold values from -0.1875 to 0.1875
- w_up: bfloat16 [8, 896, 4864], P('grp', None, 'mem'), may hold values from -0.1875 to 0.1875
- w_down: bfloat16 [8, 4864, 896], P('grp', 'mem'), may hold values from -0.078125 to 0.078125
- out_grad: bfloat16 [8, 4, 128, 896], P('grp', 'mem'), may hold values from -6 to 6
- valid: int32 [8, 4], P('grp', 'mem'), may hold values from 64 to 128
Outputs:
- server_out: bfloat16 [8, 4, 128, 896], P('grp', 'mem')
- grad_query: bfloat16 [4, 896, 896], P('mem')
- grad_keyval: bfloat16 [4, 896, 256], P('mem')
- grad_out: bfloat16 [4, 896, 896], P('mem')
- grad_gate: bfloat16 [8, 896, 4864], P('grp', None, 'mem')
- grad_up: bfloat16 [8, 896, 4864], P('grp', None, 'mem')
- grad_down: bfloat16 [8, 4864, 896], P('grp', 'mem')
The draws below stay inside these ranges and needn't reach their ends.
All inputs are finite; a program needn't handle non-finite values.
Results may differ from the reference program's by a relative error of at most 0.03.
Values may be sent and summed in bfloat16 or wider, within the bound.
A program may use at most 128 MiB of HBM per device.

```python
import jax
import jax.numpy as jnp
from jax import lax

D = 896
FF = 4864
KV_HEADS = 2
HEAD_DIM = 64
TOK = 128
GROUPS = 8
MEMBERS = 4


def query_tables(key):
    first, second = jax.random.split(jax.random.fold_in(key, 11))
    scale = D ** (-0.5)
    keyval = jax.random.normal(first, (MEMBERS, D, 2 * KV_HEADS * HEAD_DIM), jnp.float32) * scale
    query = jax.random.normal(second, (MEMBERS, D, D), jnp.float32) * scale
    return (jnp.clip(query, -1.5, 1.5), jnp.clip(keyval, -0.5, 0.5))


def draw_w_query(key, part):
    return query_tables(key)[0].astype(jnp.bfloat16)


def draw_w_keyval(key, part):
    return query_tables(key)[1].astype(jnp.bfloat16)


def touch_ends(drawn, stream_key, least, high):
    dims = drawn.shape
    index_at = [jax.random.randint(jax.random.fold_in(stream_key, axis), (), 0, dims[axis]) for axis in range(len(dims))]
    drawn = drawn.at[tuple(index_at)].set(least)
    longest = dims.index(max(dims))
    index_at[longest] = (index_at[longest] + 1) % dims[longest]
    return drawn.at[tuple(index_at)].set(high)


def shard_levels(key, extent, pieces, smallest, largest):
    gain, own = 1.0, jax.random.fold_in(key, 6)
    for axis_at, shards_of in pieces:
        steps = jnp.exp(jax.random.uniform(jax.random.fold_in(own, axis_at), (shards_of,), jnp.float32, smallest / len(pieces), largest / len(pieces)))
        gain = gain * jnp.repeat(steps, extent[axis_at] // shards_of).reshape([-1 if axis == axis_at else 1 for axis in range(len(extent))])
    return gain


def scatter_about(own_key, dims, scale, limit, pieces=(), held_as=jnp.bfloat16):
    values = scale * jax.random.normal(own_key, dims, jnp.float32)
    if pieces:
        values = values * shard_levels(own_key, dims, pieces, -0.22, 0.18)
    return jnp.clip(values, -limit, limit).astype(held_as)


def setup_inputs(seed: int = 0) -> dict:
    keys = jax.random.split(jax.random.key(seed), 12)
    return {
        "client_input": scatter_about(keys[0], (GROUPS, MEMBERS, TOK, D), 1.0, 6.0, ((0, 8), (1, 4))),
        "client_gain": jnp.clip(1.0 + 0.1 * jax.random.normal(keys[1], (MEMBERS, D), jnp.float32), 0.5, 1.5),
        "w_query": draw_w_query(jax.random.fold_in(keys[11], 71), 0),
        "w_keyval": draw_w_keyval(jax.random.fold_in(keys[11], 71), 0),
        "w_out": scatter_about(keys[4], (MEMBERS, D, D), D ** -0.5, 0.1875, ((0, 4),)),
        "server_gain": jnp.clip(1.0 + 0.1 * jax.random.normal(keys[5], (GROUPS, D), jnp.float32), 0.5, 1.5),
        "w_gate": scatter_about(keys[6], (GROUPS, D, FF), D ** -0.5, 0.1875, ((0, 8), (2, 4))),
        "w_up": scatter_about(keys[7], (GROUPS, D, FF), D ** -0.5, 0.1875, ((0, 8), (2, 4))),
        "w_down": scatter_about(keys[8], (GROUPS, FF, D), FF ** -0.5, 0.078125, ((0, 8), (1, 4))),
        "out_grad": scatter_about(keys[9], (GROUPS, MEMBERS, TOK, D), 1.0, 6.0, ((0, 8), (1, 4))),
        "valid": touch_ends(jax.random.randint(keys[10], (GROUPS, MEMBERS), TOK // 2, TOK + 1), jax.random.fold_in(keys[10], 1), TOK // 2, TOK).astype(jnp.int32),
    }


EPS = 1e-06

def client_forward(tokens_in, gain_vec, query_w, keyval_w, output_w):
    x_float = tokens_in.astype(jnp.float32)
    inv_rms = lax.rsqrt(lax.optimization_barrier(jnp.mean(x_float * x_float, axis=-1, keepdims=True)) + EPS)
    normed = (x_float * inv_rms * gain_vec).astype(jnp.bfloat16)
    queries = jnp.dot(normed, query_w, preferred_element_type=jnp.float32).astype(jnp.bfloat16)
    key_vals = jnp.dot(normed, keyval_w, preferred_element_type=jnp.float32).astype(jnp.bfloat16)
    length = tokens_in.shape[0]
    half_cols = KV_HEADS * HEAD_DIM
    q_heads = queries.reshape(length, KV_HEADS, -1, HEAD_DIM)
    k_heads = key_vals[:, :half_cols].reshape(length, KV_HEADS, HEAD_DIM)
    v_heads = key_vals[:, half_cols:].reshape(length, KV_HEADS, HEAD_DIM)
    scores = jnp.einsum('tgqd,sgd->gqts', q_heads.astype(jnp.float32), k_heads.astype(jnp.float32)) * HEAD_DIM ** (-0.5)
    causal = jnp.arange(length)[:, None] >= jnp.arange(length)[None, :]
    scores = jnp.where(causal, scores, -1e+30)
    highest = lax.optimization_barrier(jnp.max(scores, axis=-1, keepdims=True))
    expo = jnp.exp(scores - highest)
    probs = (expo / lax.optimization_barrier(jnp.sum(expo, axis=-1, keepdims=True))).astype(jnp.bfloat16)
    attended = jnp.einsum('gqts,sgd->tgqd', probs.astype(jnp.float32), v_heads.astype(jnp.float32))
    attended = attended.astype(jnp.bfloat16).reshape(length, -1)
    mixed = jnp.dot(attended, output_w, preferred_element_type=jnp.float32)
    return (x_float + mixed).astype(jnp.bfloat16)

def client_gradients(tokens_in, gain_vec, query_w, keyval_w, output_w, upstream):

    def inner(query_in, keyval_in, output_in):
        return client_forward(tokens_in, gain_vec, query_in, keyval_in, output_in)
    _, pull = jax.vjp(inner, query_w, keyval_w, output_w)
    return pull(upstream)

def norm_back(h_float, inv_rms, gain_vec, upstream):
    scaled = upstream * gain_vec
    return inv_rms * scaled - h_float * inv_rms ** 3 * lax.optimization_barrier(jnp.mean(scaled * h_float, axis=-1, keepdims=True))

def reference(client_input, client_gain, w_query, w_keyval, w_out, server_gain, w_gate, w_up, w_down, out_grad, valid):
    groups = client_input.shape[0]
    members = client_input.shape[1]
    length = client_input.shape[2]
    width = client_input.shape[3]
    positions = jnp.arange(length).astype(jnp.int32)

    def group_step(totals, group_in):
        x_group, s_gain, gate_w, up_w, down_w, cot_group, valid_group = group_in
        cuts = jax.vmap(client_forward)(x_group, client_gain, w_query, w_keyval, w_out)
        rows_cut = cuts.reshape(-1, width)
        h_float = rows_cut.astype(jnp.float32)
        inv_rms = lax.rsqrt(lax.optimization_barrier(jnp.mean(h_float * h_float, axis=-1, keepdims=True)) + EPS)
        normed = (h_float * inv_rms * s_gain).astype(jnp.bfloat16)
        gate_act = jnp.dot(normed, gate_w, preferred_element_type=jnp.float32)
        up_act = jnp.dot(normed, up_w, preferred_element_type=jnp.float32)
        sigma = jax.nn.sigmoid(gate_act)
        hidden = (gate_act * sigma * up_act).astype(jnp.bfloat16)
        server_rows = (h_float + jnp.dot(hidden, down_w, preferred_element_type=jnp.float32)).astype(jnp.bfloat16)
        live = positions[None, :] < valid_group[:, None]
        cot_rows = jnp.where(live[:, :, None], cot_group, jnp.zeros_like(cot_group)).reshape(-1, width)
        d_hidden = jnp.dot(cot_rows, down_w.T, preferred_element_type=jnp.float32)
        d_gate = (d_hidden * up_act * sigma * (1.0 + gate_act * (1.0 - sigma))).astype(jnp.bfloat16)
        d_up = (d_hidden * gate_act * sigma).astype(jnp.bfloat16)
        grad_down = jnp.dot(hidden.T, cot_rows, preferred_element_type=jnp.float32).astype(jnp.bfloat16)
        grad_gate = jnp.dot(normed.T, d_gate, preferred_element_type=jnp.float32).astype(jnp.bfloat16)
        grad_up = jnp.dot(normed.T, d_up, preferred_element_type=jnp.float32).astype(jnp.bfloat16)
        d_normed = jnp.dot(d_gate, gate_w.T, preferred_element_type=jnp.float32) + jnp.dot(d_up, up_w.T, preferred_element_type=jnp.float32)
        d_cut = cot_rows.astype(jnp.float32) + norm_back(h_float, inv_rms, s_gain, d_normed)
        cut_grad = (lax.optimization_barrier(jnp.sum(d_cut.reshape(members, length, width), axis=0)) / members).astype(jnp.bfloat16)
        grads = jax.vmap(client_gradients, in_axes=(0, 0, 0, 0, 0, None))(x_group, client_gain, w_query, w_keyval, w_out, cut_grad)
        new_totals = tuple((total + lax.optimization_barrier(piece).astype(jnp.float32) for total, piece in zip(totals, grads)))
        return (new_totals, (server_rows.reshape(members, length, width), grad_gate, grad_up, grad_down))
    start = (jnp.zeros(w_query.shape, jnp.float32), jnp.zeros(w_keyval.shape, jnp.float32), jnp.zeros(w_out.shape, jnp.float32))
    totals, stacked = lax.scan(group_step, start, (client_input, server_gain, w_gate, w_up, w_down, out_grad, valid))
    server_out, grad_gate, grad_up, grad_down = stacked
    grad_query = (totals[0] / groups).astype(jnp.bfloat16)
    grad_keyval = (totals[1] / groups).astype(jnp.bfloat16)
    grad_out = (totals[2] / groups).astype(jnp.bfloat16)
    return (server_out, grad_query, grad_keyval, grad_out, grad_gate, grad_up, grad_down)
```

```python
import jax
import jax.numpy as jnp
from jax import lax
from jax.sharding import PartitionSpec as P

KV_HEADS = 2
HEAD_DIM = 64


EPS = 1e-06
F32 = jnp.float32
BF16 = jnp.bfloat16
CONTRACT_LAST = (((1,), (1,)), ((), ()))
CONTRACT_FIRST = (((0,), (0,)), ((), ()))


def rms(h_float):
    return lax.rsqrt(jnp.mean(h_float * h_float, axis=-1, keepdims=True) + EPS)


def norm_back(h_float, inv_rms, gain_vec, upstream):
    scaled = upstream * gain_vec
    return inv_rms * scaled - h_float * inv_rms**3 * jnp.mean(
        scaled * h_float, axis=-1, keepdims=True
    )


def attention(queries, key_vals):
    length = queries.shape[0]
    half_cols = KV_HEADS * HEAD_DIM
    q_heads = queries.reshape(length, KV_HEADS, -1, HEAD_DIM)
    k_heads = key_vals[:, :half_cols].reshape(length, KV_HEADS, HEAD_DIM)
    v_heads = key_vals[:, half_cols:].reshape(length, KV_HEADS, HEAD_DIM)
    scores = jnp.einsum(
        "tgqd,sgd->gqts", q_heads, k_heads, preferred_element_type=F32
    ) * HEAD_DIM ** (-0.5)
    causal = jnp.arange(length)[:, None] >= jnp.arange(length)[None, :]
    scores = jnp.where(causal, scores, -1e30)
    highest = jnp.max(scores, axis=-1, keepdims=True)
    expo = jnp.exp(scores - highest)
    probs = (expo / jnp.sum(expo, axis=-1, keepdims=True)).astype(BF16)
    attended = jnp.einsum("gqts,sgd->tgqd", probs, v_heads, preferred_element_type=F32)
    return attended.astype(BF16).reshape(length, -1)


def flip(block, axis):
    n = lax.axis_size(axis)
    return lax.ppermute(block, axis, [(i, i ^ 1) for i in range(n)])


def ring(block, axis):
    n = lax.axis_size(axis)
    return lax.ppermute(block, axis, [(i, (i + 2) % n) for i in range(n)])


def gather_groups(block):
    pairs = lax.axis_size("grp") // 2
    blocks = []
    for step in range(pairs):
        blocks += [block, flip(block, "grp")]
        if step < pairs - 1:
            block = ring(block, "grp")
    return blocks


def gather_members(block):
    pairs = lax.axis_size("mem") // 2
    singles = [block]
    for _ in range(pairs - 1):
        singles.append(ring(singles[-1], "mem"))
    both = flip(jnp.concatenate(singles, axis=0), "mem")
    return jnp.concatenate(singles + [both], axis=0)


def on_device(
    client_input,
    client_gain,
    w_query,
    w_keyval,
    w_out,
    server_gain,
    w_gate,
    w_up,
    w_down,
    out_grad,
    valid,
):
    tokens_in = client_input[0, 0]
    query_w = w_query[0]
    keyval_w = w_keyval[0]
    output_w = w_out[0]
    s_gain = server_gain[0]
    gate_w = w_gate[0]
    up_w = w_up[0]
    down_w = w_down[0]
    length, width = tokens_in.shape
    members = lax.axis_size("mem")
    groups = lax.axis_size("grp")
    pairs = members // 2
    half = length // 2
    odd = lax.axis_index("mem") % 2

    live = jnp.arange(length) < valid[0, 0]
    own_cot = jnp.where(live[:, None], out_grad[0, 0], jnp.zeros_like(out_grad[0, 0]))
    all_cot = gather_members(own_cot)

    x_float = tokens_in.astype(F32)
    client_normed = (x_float * rms(x_float) * client_gain[0]).astype(BF16)
    queries = jnp.dot(client_normed, query_w, preferred_element_type=F32).astype(BF16)
    key_vals = jnp.dot(client_normed, keyval_w, preferred_element_type=F32).astype(BF16)
    attended, pull = jax.vjp(attention, queries, key_vals)
    mixed = jnp.dot(attended, output_w, preferred_element_type=F32)
    own_cut = (x_float + mixed).astype(BF16)

    all_cut = gather_members(own_cut)
    normed_groups = gather_groups(client_normed)
    attended_groups = gather_groups(attended)
    h_float = all_cut.astype(F32)
    inv_rms = rms(h_float)
    normed = (h_float * inv_rms * s_gain).astype(BF16)
    d_hidden = lax.dot_general(all_cot, down_w, CONTRACT_LAST, preferred_element_type=F32)
    gate_act = jnp.dot(normed, gate_w, preferred_element_type=F32)
    up_act = jnp.dot(normed, up_w, preferred_element_type=F32)
    sigma = jax.nn.sigmoid(gate_act)
    hidden = (gate_act * sigma * up_act).astype(BF16)
    d_gate = (d_hidden * up_act * sigma * (1.0 + gate_act * (1.0 - sigma))).astype(BF16)
    d_up = (d_hidden * gate_act * sigma).astype(BF16)
    d_normed = lax.dot_general(d_gate, gate_w, CONTRACT_LAST, preferred_element_type=F32)
    d_normed = d_normed + lax.dot_general(d_up, up_w, CONTRACT_LAST, preferred_element_type=F32)
    pushed = norm_back(h_float, inv_rms, s_gain, d_normed)
    local_sum = jnp.sum(pushed.reshape(-1, length, width), axis=0) + own_cot.astype(F32)

    keep = lax.dynamic_slice_in_dim(local_sum, odd * half, half, 0)
    give = lax.dynamic_slice_in_dim(local_sum, (1 - odd) * half, half, 0).astype(BF16)
    part = keep + flip(give, "mem").astype(F32)
    total = part
    passing = part.astype(BF16)
    for _ in range(pairs - 1):
        passing = ring(passing, "mem")
        total = total + passing.astype(F32)
    half_grad = (total / members).astype(BF16)
    half_groups = gather_groups(half_grad)
    other_half = flip(half_grad, "mem")

    def whole(mine, other):
        return jnp.where(
            odd == 0, jnp.concatenate([mine, other]), jnp.concatenate([other, mine])
        )

    cut_grad = whole(half_grad, other_half)

    d_attended = lax.dot_general(
        cut_grad, output_w, CONTRACT_LAST, preferred_element_type=F32
    ).astype(BF16)
    d_queries, d_key_vals = pull(d_attended)
    d_groups = gather_groups(jnp.concatenate([d_queries, d_key_vals], axis=1))

    grad_down = lax.dot_general(
        hidden, all_cot, CONTRACT_FIRST, preferred_element_type=F32
    ).astype(BF16)
    grad_gate = lax.dot_general(
        normed, d_gate, CONTRACT_FIRST, preferred_element_type=F32
    ).astype(BF16)
    grad_up = lax.dot_general(
        normed, d_up, CONTRACT_FIRST, preferred_element_type=F32
    ).astype(BF16)
    served = jnp.dot(hidden, down_w, preferred_element_type=F32).astype(BF16)
    served = served.reshape(2, pairs, length, width)
    mine = served[0].astype(F32) + flip(served[1], "mem").astype(F32)
    result = mine[0]
    n = members
    for p in range(1, pairs):
        home = lax.ppermute(
            mine[p].astype(BF16), "mem", [(i, (i - 2 * p) % n) for i in range(n)]
        )
        result = result + home.astype(F32)
    server_out = (own_cut.astype(F32) + result).astype(BF16)

    all_halves = jnp.stack(half_groups)
    other_halves = flip(all_halves, "mem")
    all_grads = jnp.where(
        odd == 0,
        jnp.concatenate([all_halves, other_halves], axis=1),
        jnp.concatenate([other_halves, all_halves], axis=1),
    ).reshape(-1, width)
    grad_out = lax.dot_general(
        jnp.concatenate(attended_groups), all_grads, CONTRACT_FIRST, preferred_element_type=F32
    )
    grad_in = lax.dot_general(
        jnp.concatenate(normed_groups),
        jnp.concatenate(d_groups),
        CONTRACT_FIRST,
        preferred_element_type=F32,
    )
    grad_out = (grad_out / groups).astype(BF16)
    grad_query = (grad_in[:, : queries.shape[1]] / groups).astype(BF16)
    grad_keyval = (grad_in[:, queries.shape[1] :] / groups).astype(BF16)
    return (
        server_out[None, None],
        grad_query[None],
        grad_keyval[None],
        grad_out[None],
        grad_gate[None],
        grad_up[None],
        grad_down[None],
    )


def solution(mesh):
    in_specs = (
        P("grp", "mem", None, None),
        P("mem", None),
        P("mem", None, None),
        P("mem", None, None),
        P("mem", None, None),
        P("grp", None),
        P("grp", None, "mem"),
        P("grp", None, "mem"),
        P("grp", "mem", None),
        P("grp", "mem", None, None),
        P("grp", "mem"),
    )
    out_specs = (
        P("grp", "mem", None, None),
        P("mem", None, None),
        P("mem", None, None),
        P("mem", None, None),
        P("grp", None, "mem"),
        P("grp", None, "mem"),
        P("grp", "mem", None),
    )
    return jax.shard_map(
        on_device, mesh=mesh, in_specs=in_specs, out_specs=out_specs, check_vma=False
    )
```

```python
import jax
import jax.numpy as jnp
from jax import lax
from jax.experimental import pallas as pl
from jax.experimental.pallas import tpu as pltpu
from jax.sharding import PartitionSpec as P

KV_HEADS = 2
HEAD_DIM = 64


EPS = 1e-06
F32 = jnp.float32
BF16 = jnp.bfloat16
CONTRACT_LAST = (((1,), (1,)), ((), ()))
CONTRACT_FIRST = (((0,), (0,)), ((), ()))


def rms(h_float):
    return lax.rsqrt(jnp.mean(h_float * h_float, axis=-1, keepdims=True) + EPS)


def norm_back(h_float, inv_rms, gain_vec, upstream):
    scaled = upstream * gain_vec
    return inv_rms * scaled - h_float * inv_rms**3 * jnp.mean(
        scaled * h_float, axis=-1, keepdims=True
    )


def attention(queries, key_vals):
    length = queries.shape[0]
    half_cols = KV_HEADS * HEAD_DIM
    q_heads = queries.reshape(length, KV_HEADS, -1, HEAD_DIM)
    k_heads = key_vals[:, :half_cols].reshape(length, KV_HEADS, HEAD_DIM)
    v_heads = key_vals[:, half_cols:].reshape(length, KV_HEADS, HEAD_DIM)
    scores = jnp.einsum(
        "tgqd,sgd->gqts", q_heads, k_heads, preferred_element_type=F32
    ) * HEAD_DIM ** (-0.5)
    causal = jnp.arange(length)[:, None] >= jnp.arange(length)[None, :]
    scores = jnp.where(causal, scores, -1e30)
    highest = jnp.max(scores, axis=-1, keepdims=True)
    expo = jnp.exp(scores - highest)
    probs = (expo / jnp.sum(expo, axis=-1, keepdims=True)).astype(BF16)
    attended = jnp.einsum("gqts,sgd->tgqd", probs, v_heads, preferred_element_type=F32)
    return attended.astype(BF16).reshape(length, -1)


MESH = pl.DeviceIdType.MESH


class Gather:
    def __init__(self, axis, own, slots, sems):
        self.axis, self.own, self.slots, self.sems = axis, own, slots, sems
        self.n = lax.axis_size(axis)
        self.pairs = self.n // 2
        me = lax.axis_index(axis)
        self.right = {axis: lax.rem(me + 2, self.n)}
        self.partner = {axis: me + 1 - 2 * lax.rem(me, 2)}

    def source(self, step):
        return self.own if step == 0 else self.slots.at[2 * step]

    def ring_copy(self, step):
        ring_send, ring_recv = self.sems[0], self.sems[1]
        return pltpu.make_async_remote_copy(
            src_ref=self.source(step),
            dst_ref=self.slots.at[2 * step + 2],
            send_sem=ring_send.at[step],
            recv_sem=ring_recv.at[step],
            device_id=self.right,
            device_id_type=MESH,
        )

    def flip_copy(self, step):
        return pltpu.make_async_remote_copy(
            src_ref=self.source(step),
            dst_ref=self.slots.at[2 * step + 1],
            send_sem=self.sems[2].at[step],
            recv_sem=self.sems[3].at[step],
            device_id=self.partner,
            device_id_type=MESH,
        )

    def advance(self, step):
        if step > 0:
            self.ring_copy(step - 1).wait_recv()
        if step < self.pairs - 1:
            self.ring_copy(step).start()
        self.flip_copy(step).start()

    def take(self, step):
        self.flip_copy(step).wait_recv()

    def finish(self):
        for step in range(self.pairs):
            if step < self.pairs - 1:
                self.ring_copy(step).wait_send()
            self.flip_copy(step).wait_send()


def gather_sems(n):
    pairs = n // 2
    return [
        pltpu.SemaphoreType.DMA((max(pairs - 1, 1),)),
        pltpu.SemaphoreType.DMA((max(pairs - 1, 1),)),
        pltpu.SemaphoreType.DMA((pairs,)),
        pltpu.SemaphoreType.DMA((pairs,)),
    ]


def greet(axes):
    barrier = pltpu.get_barrier_semaphore()
    count = 0
    for axis in axes:
        n = lax.axis_size(axis)
        me = lax.axis_index(axis)
        pl.semaphore_signal(
            barrier, 1, device_id={axis: me + 1 - 2 * lax.rem(me, 2)}, device_id_type=MESH
        )
        for k in range(1, n // 2):
            pl.semaphore_signal(
                barrier, 1, device_id={axis: lax.rem(me + 2 * k, n)}, device_id_type=MESH
            )
        count += n // 2
    pl.semaphore_wait(barrier, count)


def send(src, dst, sems, index, device):
    return pltpu.make_async_remote_copy(
        src_ref=src,
        dst_ref=dst,
        send_sem=sems[0].at[index],
        recv_sem=sems[1].at[index],
        device_id=device,
        device_id_type=MESH,
    )


def server_kernel(
    cut_own, cot_own, attended_own, normed_own, gain, gate_hbm, up_hbm, down_hbm,
    server_out, cut_grad, attended_all, normed_all, rows_normed, rows_cot, hidden, d_gate, d_up,
    gate_w, up_w, down_w, cut_slots, served, served_in, home_in, home_out, sums, give, give_in,
    passing, pass_in, load_sem, cut_sems, cot_sems, attended_sems, normed_sems, swap_sems, part_sems,
    home_sems, pass_sems,
):
    members, groups = lax.axis_size("mem"), lax.axis_size("grp")
    pairs, group_pairs = members // 2, groups // 2
    length, width = cut_own.shape
    half = length // 2
    me = lax.axis_index("mem")
    odd = lax.rem(me, 2)
    partner = {"mem": me + 1 - 2 * odd}
    loads = []
    for i, (far, near) in enumerate(((down_hbm, down_w), (gate_hbm, gate_w), (up_hbm, up_w))):
        loads.append(pltpu.make_async_copy(far, near, load_sem.at[i]))
        loads[-1].start()
    greet(("grp", "mem"))
    cut = Gather("mem", cut_own, cut_slots, cut_sems)
    cot = Gather("mem", cot_own, rows_cot, cot_sems)
    early = [
        Gather("grp", normed_own, normed_all, normed_sems),
        Gather("grp", attended_own, attended_all, attended_sems),
    ]
    cut.advance(0)
    cot.advance(0)
    for chain in early:
        chain.advance(0)
    cut_slots[0] = cut_own[...]
    rows_cot[0] = cot_own[...]
    normed_all[0] = normed_own[...]
    attended_all[0] = attended_own[...]
    sums[...] = cot_own[...].astype(F32)
    swaps = []
    group_step = 1
    for p in range(pairs):
        if p > 0:
            cut.advance(p)
            cot.advance(p)
        cut.take(p)
        cot.take(p)
        span = pl.ds(2 * p, 2)
        h_float = cut_slots[span].reshape(2 * length, width).astype(F32)
        inv_rms = rms(h_float)
        normed = (h_float * inv_rms * gain[...]).astype(BF16)
        rows_normed[span] = normed.reshape(2, length, width)
        if p == 0:
            for load in loads:
                load.wait()
        d_hidden = lax.dot_general(
            rows_cot[span].reshape(2 * length, width), down_w[...], CONTRACT_LAST,
            preferred_element_type=F32,
        )
        gate_act = lax.dot_general(normed, gate_w[...], CONTRACT_LAST, preferred_element_type=F32)
        up_act = lax.dot_general(normed, up_w[...], CONTRACT_LAST, preferred_element_type=F32)
        sigma = jax.nn.sigmoid(gate_act)
        acted = gate_act * sigma
        hidden_now = (acted * up_act).astype(BF16)
        dg = (d_hidden * up_act * sigma * (1.0 + gate_act * (1.0 - sigma))).astype(BF16)
        du = (d_hidden * acted).astype(BF16)
        rows = pl.ds(2 * p * length, 2 * length)
        hidden[rows] = hidden_now
        d_gate[rows] = dg
        d_up[rows] = du
        d_normed = jnp.dot(dg, gate_w[...], preferred_element_type=F32)
        d_normed = d_normed + jnp.dot(du, up_w[...], preferred_element_type=F32)
        pushed = norm_back(h_float, inv_rms, gain[...], d_normed)
        sums[...] += pushed[:length] + pushed[length:]
        served[span] = (
            jnp.dot(hidden_now, down_w[...], preferred_element_type=F32)
            .astype(BF16)
            .reshape(2, length, width)
        )
        if group_step < group_pairs - 1:
            for chain in early:
                chain.advance(group_step)
            group_step += 1

    keep_rows = pl.ds(pl.multiple_of(odd * half, half), half)
    give_rows = pl.ds(pl.multiple_of((1 - odd) * half, half), half)
    give[...] = sums[give_rows].astype(BF16)
    handed = send(give, give_in, part_sems, 0, partner)
    handed.start()
    for p in range(pairs):
        swaps.append(send(served.at[2 * p + 1], served_in.at[p], swap_sems, p, partner))
        swaps[-1].start()
    handed.wait_recv()
    total = sums[keep_rows] + give_in[...].astype(F32)
    passing[...] = total.astype(BF16)
    passes = []
    for k in range(1, pairs):
        passes.append(
            send(passing, pass_in.at[k - 1], pass_sems, k - 1, {"mem": lax.rem(me + 2 * k, members)})
        )
        passes[-1].start()
    homes = []
    for p in range(pairs):
        swaps[p].wait_recv()
        mine = served[2 * p].astype(F32) + served_in[p].astype(F32)
        if p == 0:
            result = cut_own[...].astype(F32) + mine
            sums[...] = result
        else:
            home_out[p - 1] = mine.astype(BF16)
            homes.append(
                send(
                    home_out.at[p - 1], home_in.at[p - 1], home_sems, p - 1,
                    {"mem": lax.rem(me + members - 2 * p, members)},
                )
            )
            homes[-1].start()
    for k in range(1, pairs):
        passes[k - 1].wait_recv()
        total = total + pass_in[k - 1].astype(F32)
    cut_grad[keep_rows] = (total / members).astype(BF16)
    back = send(cut_grad.at[keep_rows], cut_grad.at[keep_rows], part_sems, 1, partner)
    back.start()
    result = sums[...]
    for p in range(1, pairs):
        homes[p - 1].wait_recv()
        result = result + home_in[p - 1].astype(F32)
    server_out[...] = result.astype(BF16)
    while group_step < group_pairs:
        for chain in early:
            chain.advance(group_step)
        group_step += 1
    for chain in early:
        for step in range(group_pairs):
            chain.take(step)
        chain.finish()
    cut.finish()
    cot.finish()
    back.wait_recv()
    for copy in [handed, back] + swaps + passes + homes:
        copy.wait_send()


def server_call(cut, cot, attended, normed, gain, gate_t, up_t, down):
    members, groups = lax.axis_size("mem"), lax.axis_size("grp")
    pairs = members // 2
    length, width = cut.shape
    units = down.shape[0]
    half = length // 2
    rows = members * length
    shape = jax.ShapeDtypeStruct
    vmem = pl.BlockSpec(memory_space=pltpu.VMEM)
    far = pl.BlockSpec(memory_space=pl.ANY)
    others = max(pairs - 1, 1)
    two = lambda count: [pltpu.SemaphoreType.DMA((count,))] * 2
    return pl.pallas_call(
        server_kernel,
        out_shape=[
            shape((length, width), BF16),
            shape((length, width), BF16),
            shape((groups, length, width), BF16),
            shape((groups, length, width), BF16),
            shape((members, length, width), BF16),
            shape((members, length, width), BF16),
            shape((rows, units), BF16),
            shape((rows, units), BF16),
            shape((rows, units), BF16),
        ],
        in_specs=[vmem] * 5 + [far] * 3,
        out_specs=[vmem] * 9,
        scratch_shapes=[
            pltpu.VMEM((units, width), BF16),
            pltpu.VMEM((units, width), BF16),
            pltpu.VMEM((units, width), BF16),
            pltpu.VMEM((members, length, width), BF16),
            pltpu.VMEM((members, length, width), BF16),
            pltpu.VMEM((pairs, length, width), BF16),
            pltpu.VMEM((others, length, width), BF16),
            pltpu.VMEM((others, length, width), BF16),
            pltpu.VMEM((length, width), F32),
            pltpu.VMEM((half, width), BF16),
            pltpu.VMEM((half, width), BF16),
            pltpu.VMEM((half, width), BF16),
            pltpu.VMEM((others, half, width), BF16),
            pltpu.SemaphoreType.DMA((3,)),
            gather_sems(members),
            gather_sems(members),
            gather_sems(groups),
            gather_sems(groups),
            two(pairs),
            two(2),
            two(others),
            two(others),
        ],
        compiler_params=pltpu.CompilerParams(
            collective_id=0, has_side_effects=True, vmem_limit_bytes=60 * 2**20
        ),
        name="server",
    )(cut, cot, attended, normed, gain, gate_t, up_t, down)


def grads_kernel(
    d_own, half_own, attended_all, normed_all, rows_normed, rows_cot, hidden, d_gate, d_up,
    grad_in, grad_out, grad_gate, grad_up, grad_down,
    d_slots, half_slots, half_in, acc, d_sems, half_sems, swap_sems,
):
    groups = lax.axis_size("grp")
    group_pairs = groups // 2
    half, width = half_own.shape
    length = 2 * half
    rows = rows_cot.shape[0] * length
    me = lax.axis_index("mem")
    odd = lax.rem(me, 2)
    partner = {"mem": me + 1 - 2 * odd}
    greet(("grp", "mem"))
    halves = Gather("grp", half_own, half_slots, half_sems)
    deltas = Gather("grp", d_own, d_slots, d_sems)
    chains = [halves, deltas]
    for chain in chains:
        chain.advance(0)
    half_slots[0] = half_own[...]
    d_slots[0] = d_own[...]
    acc_rows = acc.shape[0] // 2

    def weight_grad(left, right, out):
        right_now = right
        units = out.shape[0]
        out[...] = lax.dot_general(
            left[...], right_now, CONTRACT_FIRST, preferred_element_type=F32
        ).astype(BF16)

    cot = rows_cot[...].reshape(rows, width)
    normed = rows_normed[...].reshape(rows, width)
    jobs = [(hidden, cot, grad_down), (d_gate, normed, grad_gate), (d_up, normed, grad_up)]
    for step in range(1, group_pairs):
        if jobs:
            weight_grad(*jobs.pop(0))
        for chain in chains:
            chain.advance(step)
    while jobs:
        weight_grad(*jobs.pop(0))
    for step in range(group_pairs):
        halves.take(step)
    swap = send(half_slots, half_in, swap_sems, 0, partner)
    swap.start()
    ready = groups - 2
    for step in range(group_pairs - 1):
        deltas.take(step)
    scale = 1.0 / groups
    acc[...] = lax.dot_general(
        normed_all[pl.ds(0, ready)].reshape(ready * length, width),
        d_slots[pl.ds(0, ready)].reshape(ready * length, d_slots.shape[2]),
        CONTRACT_FIRST,
        preferred_element_type=F32,
    )
    swap.wait_recv()
    mine = half_slots[...]
    other = half_in[...]
    top = jnp.where(odd == 0, mine, other)
    bottom = jnp.where(odd == 0, other, mine)
    top_att = attended_all[:, pl.ds(0, half), :].reshape(groups * half, width)
    low_att = attended_all[:, pl.ds(half, half), :].reshape(groups * half, width)
    out = lax.dot_general(
        top_att, top.reshape(groups * half, width), CONTRACT_FIRST, preferred_element_type=F32
    )
    out = out + lax.dot_general(
        low_att, bottom.reshape(groups * half, width), CONTRACT_FIRST, preferred_element_type=F32
    )
    grad_out[...] = (out * scale).astype(BF16)
    deltas.take(group_pairs - 1)
    last = lax.dot_general(
        normed_all[pl.ds(ready, 2)].reshape(2 * length, width),
        d_slots[pl.ds(ready, 2)].reshape(2 * length, d_slots.shape[2]),
        CONTRACT_FIRST,
        preferred_element_type=F32,
    )
    grad_in[...] = ((acc[...] + last) * scale).astype(BF16)
    for chain in chains:
        chain.finish()
    swap.wait_send()


def grads_call(d_own, half_own, attended_all, normed_all, rows_normed, rows_cot, hidden, d_gate, d_up):
    groups = lax.axis_size("grp")
    half, width = half_own.shape
    length, wide = d_own.shape
    units = hidden.shape[1]
    shape = jax.ShapeDtypeStruct
    vmem = pl.BlockSpec(memory_space=pltpu.VMEM)
    return pl.pallas_call(
        grads_kernel,
        out_shape=[
            shape((width, wide), BF16),
            shape((width, width), BF16),
            shape((units, width), BF16),
            shape((units, width), BF16),
            shape((units, width), BF16),
        ],
        in_specs=[vmem] * 9,
        out_specs=[vmem] * 5,
        scratch_shapes=[
            pltpu.VMEM((groups, length, wide), BF16),
            pltpu.VMEM((groups, half, width), BF16),
            pltpu.VMEM((groups, half, width), BF16),
            pltpu.VMEM((width, wide), F32),
            gather_sems(groups),
            gather_sems(groups),
            [pltpu.SemaphoreType.DMA((1,))] * 2,
        ],
        compiler_params=pltpu.CompilerParams(
            collective_id=1, has_side_effects=True, vmem_limit_bytes=60 * 2**20
        ),
        name="grads",
    )(d_own, half_own, attended_all, normed_all, rows_normed, rows_cot, hidden, d_gate, d_up)


def on_device(
    client_input,
    client_gain,
    w_query,
    w_keyval,
    w_out,
    server_gain,
    w_gate,
    w_up,
    w_down,
    out_grad,
    valid,
):
    tokens_in = client_input[0, 0]
    output_w = w_out[0]
    length, width = tokens_in.shape
    half = length // 2
    odd = lax.axis_index("mem") % 2
    live = jnp.arange(length) < valid[0, 0]
    own_cot = jnp.where(live[:, None], out_grad[0, 0], jnp.zeros_like(out_grad[0, 0]))

    x_float = tokens_in.astype(F32)
    client_normed = (x_float * rms(x_float) * client_gain[0]).astype(BF16)
    queries = jnp.dot(client_normed, w_query[0], preferred_element_type=F32).astype(BF16)
    key_vals = jnp.dot(client_normed, w_keyval[0], preferred_element_type=F32).astype(BF16)
    attended, pull = jax.vjp(attention, queries, key_vals)
    mixed = jnp.dot(attended, output_w, preferred_element_type=F32)
    own_cut = (x_float + mixed).astype(BF16)

    (server_out, cut_grad, attended_all, normed_all, *rest) = server_call(
        own_cut, own_cot, attended, client_normed, server_gain, w_gate[0].T, w_up[0].T, w_down[0]
    )

    d_attended = lax.dot_general(
        cut_grad, output_w, CONTRACT_LAST, preferred_element_type=F32
    ).astype(BF16)
    d_queries, d_key_vals = pull(d_attended)
    half_grad = lax.dynamic_slice_in_dim(cut_grad, odd * half, half, 0)
    grad_in, grad_out, grad_gate, grad_up, grad_down = grads_call(
        jnp.concatenate([d_queries, d_key_vals], axis=1), half_grad, attended_all, normed_all, *rest
    )
    return (
        server_out[None, None],
        grad_in[None, :, : queries.shape[1]],
        grad_in[None, :, queries.shape[1] :],
        grad_out[None],
        grad_gate.T[None],
        grad_up.T[None],
        grad_down[None],
    )


def solution(mesh):
    in_specs = (
        P("grp", "mem", None, None),
        P("mem", None),
        P("mem", None, None),
        P("mem", None, None),
        P("mem", None, None),
        P("grp", None),
        P("grp", None, "mem"),
        P("grp", None, "mem"),
        P("grp", "mem", None),
        P("grp", "mem", None, None),
        P("grp", "mem"),
    )
    out_specs = (
        P("grp", "mem", None, None),
        P("mem", None, None),
        P("mem", None, None),
        P("mem", None, None),
        P("grp", None, "mem"),
        P("grp", None, "mem"),
        P("grp", "mem", None),
    )
    return jax.shard_map(
        on_device, mesh=mesh, in_specs=in_specs, out_specs=out_specs, check_vma=False
    )
```

```python
import jax
import jax.numpy as jnp
from jax import lax
from jax.experimental import pallas as pl
from jax.experimental.pallas import tpu as pltpu
from jax.sharding import PartitionSpec as P

KV_HEADS = 2
HEAD_DIM = 64


EPS = 1e-06
F32 = jnp.float32
BF16 = jnp.bfloat16
CONTRACT_LAST = (((1,), (1,)), ((), ()))
CONTRACT_FIRST = (((0,), (0,)), ((), ()))


def rms(h_float):
    return lax.rsqrt(jnp.mean(h_float * h_float, axis=-1, keepdims=True) + EPS)


def norm_back(h_float, inv_rms, gain_vec, upstream):
    scaled = upstream * gain_vec
    return inv_rms * scaled - h_float * inv_rms**3 * jnp.mean(
        scaled * h_float, axis=-1, keepdims=True
    )


def attention(queries, key_vals):
    length = queries.shape[0]
    half_cols = KV_HEADS * HEAD_DIM
    q_heads = queries.reshape(length, KV_HEADS, -1, HEAD_DIM)
    k_heads = key_vals[:, :half_cols].reshape(length, KV_HEADS, HEAD_DIM)
    v_heads = key_vals[:, half_cols:].reshape(length, KV_HEADS, HEAD_DIM)
    scores = jnp.einsum(
        "tgqd,sgd->gqts", q_heads, k_heads, preferred_element_type=F32
    ) * HEAD_DIM ** (-0.5)
    causal = jnp.arange(length)[:, None] >= jnp.arange(length)[None, :]
    scores = jnp.where(causal, scores, -1e30)
    highest = jnp.max(scores, axis=-1, keepdims=True)
    expo = jnp.exp(scores - highest)
    probs = (expo / jnp.sum(expo, axis=-1, keepdims=True)).astype(BF16)
    attended = jnp.einsum("gqts,sgd->tgqd", probs, v_heads, preferred_element_type=F32)
    return attended.astype(BF16).reshape(length, -1)


MESH = pl.DeviceIdType.MESH


class Gather:
    def __init__(self, axis, own, slots, sems, split=False):
        self.axis, self.own, self.slots, self.sems = axis, own, slots, sems
        self.taken = set()
        self.n = lax.axis_size(axis)
        self.pairs = self.n // 2
        me = lax.axis_index(axis)
        self.right = {axis: lax.rem(me + 2, self.n)}
        self.partner = {axis: me + 1 - 2 * lax.rem(me, 2)}
        self.split = split and self.pairs > 1
        self.cut_at = own.shape[0] // 2

    def source(self, step):
        return self.own if step == 0 else self.slots.at[2 * step]

    def ring_copy(self, step):
        ring_send, ring_recv = self.sems[0], self.sems[1]
        return pltpu.make_async_remote_copy(
            src_ref=self.source(step),
            dst_ref=self.slots.at[2 * step + 2],
            send_sem=ring_send.at[step],
            recv_sem=ring_recv.at[step],
            device_id=self.right,
            device_id_type=MESH,
        )

    def rest_copy(self):
        rows = pl.ds(self.cut_at, self.own.shape[0] - self.cut_at)
        last = 2 * self.pairs - 1
        return pltpu.make_async_remote_copy(
            src_ref=self.slots.at[last - 2, rows],
            dst_ref=self.slots.at[last, rows],
            send_sem=self.sems[0].at[self.pairs - 1],
            recv_sem=self.sems[1].at[self.pairs - 1],
            device_id=self.right,
            device_id_type=MESH,
        )

    def flip_copy(self, step):
        src, dst = self.source(step), self.slots.at[2 * step + 1]
        if self.split and step == self.pairs - 1:
            rows = pl.ds(0, self.cut_at)
            src, dst = self.slots.at[2 * step, rows], self.slots.at[2 * step + 1, rows]
        return pltpu.make_async_remote_copy(
            src_ref=src,
            dst_ref=dst,
            send_sem=self.sems[2].at[step],
            recv_sem=self.sems[3].at[step],
            device_id=self.partner,
            device_id_type=MESH,
        )

    def advance(self, step):
        if step > 0:
            self.ring_copy(step - 1).wait_recv()
        if step < self.pairs - 1:
            self.ring_copy(step).start()
        self.flip_copy(step).start()
        if self.split and step == self.pairs - 1:
            self.take(step - 1)
            self.rest_copy().start()

    def take(self, step):
        if step in self.taken:
            return
        self.taken.add(step)
        self.flip_copy(step).wait_recv()
        if self.split and step == self.pairs - 1:
            self.rest_copy().wait_recv()

    def finish(self):
        for step in range(self.pairs):
            if step < self.pairs - 1:
                self.ring_copy(step).wait_send()
            self.flip_copy(step).wait_send()
        if self.split:
            self.rest_copy().wait_send()


def gather_sems(n):
    pairs = n // 2
    return [
        pltpu.SemaphoreType.DMA((pairs,)),
        pltpu.SemaphoreType.DMA((pairs,)),
        pltpu.SemaphoreType.DMA((pairs,)),
        pltpu.SemaphoreType.DMA((pairs,)),
    ]


def greet(axes):
    barrier = pltpu.get_barrier_semaphore()
    count = 0
    for axis in axes:
        n = lax.axis_size(axis)
        me = lax.axis_index(axis)
        pl.semaphore_signal(
            barrier, 1, device_id={axis: me + 1 - 2 * lax.rem(me, 2)}, device_id_type=MESH
        )
        for k in range(1, n // 2):
            pl.semaphore_signal(
                barrier, 1, device_id={axis: lax.rem(me + 2 * k, n)}, device_id_type=MESH
            )
        count += n // 2
    pl.semaphore_wait(barrier, count)


def send(src, dst, sems, index, device):
    return pltpu.make_async_remote_copy(
        src_ref=src,
        dst_ref=dst,
        send_sem=sems[0].at[index],
        recv_sem=sems[1].at[index],
        device_id=device,
        device_id_type=MESH,
    )


def server_kernel(
    cut_own, cot_own, attended_own, normed_own, gain, gate_hbm, up_hbm, down_hbm,
    server_out, cut_grad, attended_far, normed_far, rows_normed_far, rows_cot_far,
    hidden_far, d_gate_far, d_up_far,
    attended_all, normed_all, rows_normed, rows_cot, hidden, d_gate, d_up, store_sem,
    gate_w, up_w, down_w, cut_slots, served, served_in, home_in, home_out, sums, give, give_in,
    passing, pass_in, load_sem, cut_sems, cot_sems, attended_sems, normed_sems, swap_sems, part_sems,
    home_sems, pass_sems,
):
    members, groups = lax.axis_size("mem"), lax.axis_size("grp")
    pairs, group_pairs = members // 2, groups // 2
    length, width = cut_own.shape
    half = length // 2
    me = lax.axis_index("mem")
    odd = lax.rem(me, 2)
    partner = {"mem": me + 1 - 2 * odd}
    loads = []
    for i, (far, near) in enumerate(((down_hbm, down_w), (gate_hbm, gate_w), (up_hbm, up_w))):
        loads.append(pltpu.make_async_copy(far, near, load_sem.at[i]))
        loads[-1].start()
    greet(("grp", "mem"))
    cut = Gather("mem", cut_own, cut_slots, cut_sems)
    cot = Gather("mem", cot_own, rows_cot, cot_sems)
    early = [
        Gather("grp", normed_own, normed_all, normed_sems, True),
        Gather("grp", attended_own, attended_all, attended_sems, True),
    ]
    cut.advance(0)
    cot.advance(0)
    for chain in early:
        chain.advance(0)
    cut_slots[0] = cut_own[...]
    rows_cot[0] = cot_own[...]
    normed_all[0] = normed_own[...]
    attended_all[0] = attended_own[...]
    sums[...] = cot_own[...].astype(F32)
    swaps = []
    pending = [(chain, step) for step in range(1, group_pairs) for chain in early]
    stores = []

    def keep_going():
        if pending:
            chain, step = pending.pop(0)
            chain.advance(step)

    def store(near, far):
        stores.append(pltpu.make_async_copy(near, far, store_sem.at[len(stores)]))
        stores[-1].start()

    for p in range(pairs):
        if p > 0:
            cut.advance(p)
            cot.advance(p)
        cut.take(p)
        cot.take(p)
        span = pl.ds(2 * p, 2)
        h_float = cut_slots[span].reshape(2 * length, width).astype(F32)
        inv_rms = rms(h_float)
        normed = (h_float * inv_rms * gain[...]).astype(BF16)
        rows_normed[span] = normed.reshape(2, length, width)
        if p == 0:
            for load in loads:
                load.wait()
        d_hidden = lax.dot_general(
            rows_cot[span].reshape(2 * length, width), down_w[...], CONTRACT_LAST,
            preferred_element_type=F32,
        )
        gate_act = lax.dot_general(normed, gate_w[...], CONTRACT_LAST, preferred_element_type=F32)
        up_act = lax.dot_general(normed, up_w[...], CONTRACT_LAST, preferred_element_type=F32)
        keep_going()
        sigma = jax.nn.sigmoid(gate_act)
        acted = gate_act * sigma
        hidden_now = (acted * up_act).astype(BF16)
        dg = (d_hidden * up_act * sigma * (1.0 + gate_act * (1.0 - sigma))).astype(BF16)
        du = (d_hidden * acted).astype(BF16)
        rows = pl.ds(2 * p * length, 2 * length)
        hidden[rows] = hidden_now
        d_gate[rows] = dg
        d_up[rows] = du
        d_normed = jnp.dot(dg, gate_w[...], preferred_element_type=F32)
        d_normed = d_normed + jnp.dot(du, up_w[...], preferred_element_type=F32)
        pushed = norm_back(h_float, inv_rms, gain[...], d_normed)
        sums[...] += pushed[:length] + pushed[length:]
        served[span] = (
            jnp.dot(hidden_now, down_w[...], preferred_element_type=F32)
            .astype(BF16)
            .reshape(2, length, width)
        )
        keep_going()
        for near, far in (
            (hidden, hidden_far), (d_gate, d_gate_far), (d_up, d_up_far)
        ):
            store(near.at[rows], far.at[rows])
        store(rows_normed.at[span], rows_normed_far.at[span])
        store(rows_cot.at[span], rows_cot_far.at[span])

    keep_rows = pl.ds(pl.multiple_of(odd * half, half), half)
    give_rows = pl.ds(pl.multiple_of((1 - odd) * half, half), half)
    give[...] = sums[give_rows].astype(BF16)
    handed = send(give, give_in, part_sems, 0, partner)
    handed.start()
    for p in range(pairs):
        swaps.append(send(served.at[2 * p + 1], served_in.at[p], swap_sems, p, partner))
        swaps[-1].start()
    handed.wait_recv()
    keep_going()
    total = sums[keep_rows] + give_in[...].astype(F32)
    passing[...] = total.astype(BF16)
    passes = []
    for k in range(1, pairs):
        passes.append(
            send(passing, pass_in.at[k - 1], pass_sems, k - 1, {"mem": lax.rem(me + 2 * k, members)})
        )
        passes[-1].start()
    homes = []
    for p in range(pairs):
        swaps[p].wait_recv()
        mine = served[2 * p].astype(F32) + served_in[p].astype(F32)
        if p == 0:
            result = cut_own[...].astype(F32) + mine
            sums[...] = result
        else:
            home_out[p - 1] = mine.astype(BF16)
            homes.append(
                send(
                    home_out.at[p - 1], home_in.at[p - 1], home_sems, p - 1,
                    {"mem": lax.rem(me + members - 2 * p, members)},
                )
            )
            homes[-1].start()
    for k in range(1, pairs):
        passes[k - 1].wait_recv()
        total = total + pass_in[k - 1].astype(F32)
    cut_grad[keep_rows] = (total / members).astype(BF16)
    back = send(cut_grad.at[keep_rows], cut_grad.at[keep_rows], part_sems, 1, partner)
    back.start()
    result = sums[...]
    for p in range(1, pairs):
        homes[p - 1].wait_recv()
        result = result + home_in[p - 1].astype(F32)
    server_out[...] = result.astype(BF16)
    while pending:
        keep_going()
    for chain, far in zip(early, (normed_far, attended_far)):
        for step in range(group_pairs):
            chain.take(step)
        store(chain.slots, far)
    for chain in early:
        chain.finish()
    for copy in stores:
        copy.wait()
    cut.finish()
    cot.finish()
    back.wait_recv()
    for copy in [handed, back] + swaps + passes + homes:
        copy.wait_send()


def server_call(cut, cot, attended, normed, gain, gate_t, up_t, down):
    members, groups = lax.axis_size("mem"), lax.axis_size("grp")
    pairs = members // 2
    length, width = cut.shape
    units = down.shape[0]
    half = length // 2
    rows = members * length
    shape = jax.ShapeDtypeStruct
    vmem = pl.BlockSpec(memory_space=pltpu.VMEM)
    far = pl.BlockSpec(memory_space=pl.ANY)
    others = max(pairs - 1, 1)
    two = lambda count: [pltpu.SemaphoreType.DMA((count,))] * 2
    return pl.pallas_call(
        server_kernel,
        out_shape=[
            shape((length, width), BF16),
            shape((length, width), BF16),
            shape((groups, length, width), BF16),
            shape((groups, length, width), BF16),
            shape((members, length, width), BF16),
            shape((members, length, width), BF16),
            shape((rows, units), BF16),
            shape((rows, units), BF16),
            shape((rows, units), BF16),
        ],
        in_specs=[vmem] * 5 + [far] * 3,
        out_specs=[vmem] * 2 + [far] * 7,
        scratch_shapes=[
            pltpu.VMEM((groups, length, width), BF16),
            pltpu.VMEM((groups, length, width), BF16),
            pltpu.VMEM((members, length, width), BF16),
            pltpu.VMEM((members, length, width), BF16),
            pltpu.VMEM((rows, units), BF16),
            pltpu.VMEM((rows, units), BF16),
            pltpu.VMEM((rows, units), BF16),
            pltpu.SemaphoreType.DMA((5 * pairs + 2,)),
            pltpu.VMEM((units, width), BF16),
            pltpu.VMEM((units, width), BF16),
            pltpu.VMEM((units, width), BF16),
            pltpu.VMEM((members, length, width), BF16),
            pltpu.VMEM((members, length, width), BF16),
            pltpu.VMEM((pairs, length, width), BF16),
            pltpu.VMEM((others, length, width), BF16),
            pltpu.VMEM((others, length, width), BF16),
            pltpu.VMEM((length, width), F32),
            pltpu.VMEM((half, width), BF16),
            pltpu.VMEM((half, width), BF16),
            pltpu.VMEM((half, width), BF16),
            pltpu.VMEM((others, half, width), BF16),
            pltpu.SemaphoreType.DMA((3,)),
            gather_sems(members),
            gather_sems(members),
            gather_sems(groups),
            gather_sems(groups),
            two(pairs),
            two(2),
            two(others),
            two(others),
        ],
        compiler_params=pltpu.CompilerParams(
            collective_id=0, has_side_effects=True, vmem_limit_bytes=60 * 2**20
        ),
        name="server",
    )(cut, cot, attended, normed, gain, gate_t, up_t, down)


def grads_kernel(
    d_own, half_own, attended_far, normed_far, rows_normed_far, rows_cot_far,
    hidden_far, d_gate_far, d_up_far,
    grad_query, grad_keyval, grad_out, grad_gate_far, grad_up_far, grad_down_far,
    attended_all, normed_all, rows_normed, rows_cot, hidden, d_gate, d_up,
    grad_gate, grad_up, grad_down,
    d_slots, half_slots, half_in, acc, d_sems, half_sems, swap_sems, load_sem, store_sem,
):
    groups = lax.axis_size("grp")
    group_pairs = groups // 2
    half, width = half_own.shape
    length = 2 * half
    rows = rows_cot.shape[0] * length
    me = lax.axis_index("mem")
    odd = lax.rem(me, 2)
    partner = {"mem": me + 1 - 2 * odd}
    loads = []
    for i, (far, near) in enumerate((
        (hidden_far, hidden), (rows_cot_far, rows_cot), (d_gate_far, d_gate),
        (rows_normed_far, rows_normed), (d_up_far, d_up), (normed_far, normed_all),
        (attended_far, attended_all),
    )):
        loads.append(pltpu.make_async_copy(far, near, load_sem.at[i]))
        loads[-1].start()
    greet(("grp", "mem"))
    halves = Gather("grp", half_own, half_slots, half_sems, True)
    deltas = Gather("grp", d_own, d_slots, d_sems, True)
    chains = [halves, deltas]
    for chain in chains:
        chain.advance(0)
    half_slots[0] = half_own[...]
    d_slots[0] = d_own[...]
    pending = [(chain, step) for step in range(1, group_pairs) for chain in chains]

    def keep_going():
        if pending:
            chain, step = pending.pop(0)
            chain.advance(step)

    def weight_grad(left, right, out):
        out[...] = lax.dot_general(
            left[...], right[...].reshape(rows, width), CONTRACT_FIRST, preferred_element_type=F32
        ).astype(BF16)

    for load in loads:
        load.wait()
    stores = []
    for i, (left, right, near, far) in enumerate((
        (hidden, rows_cot, grad_down, grad_down_far),
        (d_gate, rows_normed, grad_gate, grad_gate_far),
        (d_up, rows_normed, grad_up, grad_up_far),
    )):
        weight_grad(left, right, near)
        stores.append(pltpu.make_async_copy(near, far, store_sem.at[i]))
        stores[-1].start()
        keep_going()
    while pending:
        keep_going()

    def grad_in(first, count):
        return lax.dot_general(
            normed_all[pl.ds(first, count)].reshape(count * length, width),
            d_slots[pl.ds(first, count)].reshape(count * length, d_slots.shape[2]),
            CONTRACT_FIRST,
            preferred_element_type=F32,
        )

    scale = 1.0 / groups
    ready = groups - 2
    for step in range(group_pairs - 1):
        deltas.take(step)
    acc[...] = grad_in(0, ready)
    for step in range(group_pairs):
        halves.take(step)
    swap = send(half_slots, half_in, swap_sems, 0, partner)
    swap.start()
    swap.wait_recv()
    mine = half_slots[...]
    other = half_in[...]
    top = jnp.where(odd == 0, mine, other)
    bottom = jnp.where(odd == 0, other, mine)
    top_att = attended_all[:, pl.ds(0, half), :].reshape(groups * half, width)
    low_att = attended_all[:, pl.ds(half, half), :].reshape(groups * half, width)
    out = lax.dot_general(
        top_att, top.reshape(groups * half, width), CONTRACT_FIRST, preferred_element_type=F32
    )
    out = out + lax.dot_general(
        low_att, bottom.reshape(groups * half, width), CONTRACT_FIRST, preferred_element_type=F32
    )
    grad_out[...] = (out * scale).astype(BF16)
    deltas.take(group_pairs - 1)
    split = grad_query.shape[1]
    result = (acc[...] + grad_in(ready, 2)) * scale
    grad_query[...] = result[:, :split].astype(BF16)
    grad_keyval[...] = result[:, split:].astype(BF16)
    for chain in chains:
        chain.finish()
    swap.wait_send()
    for copy in stores:
        copy.wait()


def grads_call(
    columns, d_own, half_own, attended_all, normed_all, rows_normed, rows_cot, hidden, d_gate, d_up
):
    groups = lax.axis_size("grp")
    half, width = half_own.shape
    length, wide = d_own.shape
    units = hidden.shape[1]
    shape = jax.ShapeDtypeStruct
    vmem = pl.BlockSpec(memory_space=pltpu.VMEM)
    far = pl.BlockSpec(memory_space=pl.ANY)
    wide_operands = [attended_all, normed_all, rows_normed, rows_cot, hidden, d_gate, d_up]
    return pl.pallas_call(
        grads_kernel,
        out_shape=[
            shape((width, columns), BF16),
            shape((width, wide - columns), BF16),
            shape((width, width), BF16),
            shape((units, width), BF16),
            shape((units, width), BF16),
            shape((units, width), BF16),
        ],
        in_specs=[vmem] * 2 + [far] * 7,
        out_specs=[vmem] * 3 + [far] * 3,
        scratch_shapes=[pltpu.VMEM(a.shape, BF16) for a in wide_operands]
        + [pltpu.VMEM((units, width), BF16)] * 3
        + [
            pltpu.VMEM((groups, length, wide), BF16),
            pltpu.VMEM((groups, half, width), BF16),
            pltpu.VMEM((groups, half, width), BF16),
            pltpu.VMEM((width, wide), F32),
            gather_sems(groups),
            gather_sems(groups),
            [pltpu.SemaphoreType.DMA((1,))] * 2,
            pltpu.SemaphoreType.DMA((7,)),
            pltpu.SemaphoreType.DMA((3,)),
        ],
        compiler_params=pltpu.CompilerParams(
            collective_id=1, has_side_effects=True, vmem_limit_bytes=60 * 2**20
        ),
        name="grads",
    )(d_own, half_own, *wide_operands)


def on_device(
    client_input,
    client_gain,
    w_query,
    w_keyval,
    w_out,
    server_gain,
    w_gate,
    w_up,
    w_down,
    out_grad,
    valid,
):
    tokens_in = client_input[0, 0]
    output_w = w_out[0]
    length, width = tokens_in.shape
    half = length // 2
    odd = lax.axis_index("mem") % 2
    live = jnp.arange(length) < valid[0, 0]
    own_cot = jnp.where(live[:, None], out_grad[0, 0], jnp.zeros_like(out_grad[0, 0]))

    x_float = tokens_in.astype(F32)
    client_normed = (x_float * rms(x_float) * client_gain[0]).astype(BF16)
    queries = jnp.dot(client_normed, w_query[0], preferred_element_type=F32).astype(BF16)
    key_vals = jnp.dot(client_normed, w_keyval[0], preferred_element_type=F32).astype(BF16)
    attended, pull = jax.vjp(attention, queries, key_vals)
    mixed = jnp.dot(attended, output_w, preferred_element_type=F32)
    own_cut = (x_float + mixed).astype(BF16)

    (server_out, cut_grad, attended_all, normed_all, *rest) = server_call(
        own_cut, own_cot, attended, client_normed, server_gain, w_gate[0].T, w_up[0].T, w_down[0]
    )

    d_attended = lax.dot_general(
        cut_grad, output_w, CONTRACT_LAST, preferred_element_type=F32
    ).astype(BF16)
    d_queries, d_key_vals = pull(d_attended)
    half_grad = lax.dynamic_slice_in_dim(cut_grad, odd * half, half, 0)
    grad_query, grad_keyval, grad_out, grad_gate, grad_up, grad_down = grads_call(
        queries.shape[1], jnp.concatenate([d_queries, d_key_vals], axis=1), half_grad, attended_all, normed_all, *rest
    )
    return (
        server_out[None, None],
        grad_query[None],
        grad_keyval[None],
        grad_out[None],
        grad_gate.T[None],
        grad_up.T[None],
        grad_down[None],
    )


def solution(mesh):
    in_specs = (
        P("grp", "mem", None, None),
        P("mem", None),
        P("mem", None, None),
        P("mem", None, None),
        P("mem", None, None),
        P("grp", None),
        P("grp", None, "mem"),
        P("grp", None, "mem"),
        P("grp", "mem", None),
        P("grp", "mem", None, None),
        P("grp", "mem"),
    )
    out_specs = (
        P("grp", "mem", None, None),
        P("mem", None, None),
        P("mem", None, None),
        P("mem", None, None),
        P("grp", None, "mem"),
        P("grp", None, "mem"),
        P("grp", "mem", None),
    )
    return jax.shard_map(
        on_device, mesh=mesh, in_specs=in_specs, out_specs=out_specs, check_vma=False
    )
```

```python
import functools

import jax
import jax.numpy as jnp
from jax import lax
from jax.experimental import pallas as pl
from jax.experimental.pallas import tpu as pltpu
from jax.sharding import PartitionSpec as P

KV_HEADS = 2
HEAD_DIM = 64


EPS = 1e-06
F32 = jnp.float32
BF16 = jnp.bfloat16
CONTRACT_LAST = (((1,), (1,)), ((), ()))
CONTRACT_FIRST = (((0,), (0,)), ((), ()))


def rms(h_float):
    return lax.rsqrt(jnp.mean(h_float * h_float, axis=-1, keepdims=True) + EPS)


def norm_back(h_float, inv_rms, gain_vec, upstream):
    scaled = upstream * gain_vec
    return inv_rms * scaled - h_float * inv_rms**3 * jnp.mean(
        scaled * h_float, axis=-1, keepdims=True
    )


def attention(queries, key_vals):
    length = queries.shape[0]
    half_cols = KV_HEADS * HEAD_DIM
    q_heads = queries.reshape(length, KV_HEADS, -1, HEAD_DIM)
    k_heads = key_vals[:, :half_cols].reshape(length, KV_HEADS, HEAD_DIM)
    v_heads = key_vals[:, half_cols:].reshape(length, KV_HEADS, HEAD_DIM)
    scores = jnp.einsum(
        "tgqd,sgd->gqts", q_heads, k_heads, preferred_element_type=F32
    ) * HEAD_DIM ** (-0.5)
    causal = jnp.arange(length)[:, None] >= jnp.arange(length)[None, :]
    scores = jnp.where(causal, scores, -1e30)
    highest = jnp.max(scores, axis=-1, keepdims=True)
    expo = jnp.exp(scores - highest)
    probs = (expo / jnp.sum(expo, axis=-1, keepdims=True)).astype(BF16)
    attended = jnp.einsum("gqts,sgd->tgqd", probs, v_heads, preferred_element_type=F32)
    return attended.astype(BF16).reshape(length, -1)


MESH = pl.DeviceIdType.MESH


class Gather:
    def __init__(self, axis, own, slots, sems, split=False):
        self.axis, self.own, self.slots, self.sems = axis, own, slots, sems
        self.taken = set()
        self.n = lax.axis_size(axis)
        self.pairs = self.n // 2
        me = lax.axis_index(axis)
        self.right = {axis: lax.rem(me + 2, self.n)}
        self.partner = {axis: me + 1 - 2 * lax.rem(me, 2)}
        self.split = split and self.pairs > 1
        self.cut_at = own.shape[0] // 2

    def source(self, step):
        return self.own if step == 0 else self.slots.at[2 * step]

    def ring_copy(self, step):
        ring_send, ring_recv = self.sems[0], self.sems[1]
        return pltpu.make_async_remote_copy(
            src_ref=self.source(step),
            dst_ref=self.slots.at[2 * step + 2],
            send_sem=ring_send.at[step],
            recv_sem=ring_recv.at[step],
            device_id=self.right,
            device_id_type=MESH,
        )

    def rest_copy(self):
        rows = pl.ds(self.cut_at, self.own.shape[0] - self.cut_at)
        last = 2 * self.pairs - 1
        return pltpu.make_async_remote_copy(
            src_ref=self.slots.at[last - 2, rows],
            dst_ref=self.slots.at[last, rows],
            send_sem=self.sems[0].at[self.pairs - 1],
            recv_sem=self.sems[1].at[self.pairs - 1],
            device_id=self.right,
            device_id_type=MESH,
        )

    def flip_copy(self, step):
        src, dst = self.source(step), self.slots.at[2 * step + 1]
        if self.split and step == self.pairs - 1:
            rows = pl.ds(0, self.cut_at)
            src, dst = self.slots.at[2 * step, rows], self.slots.at[2 * step + 1, rows]
        return pltpu.make_async_remote_copy(
            src_ref=src,
            dst_ref=dst,
            send_sem=self.sems[2].at[step],
            recv_sem=self.sems[3].at[step],
            device_id=self.partner,
            device_id_type=MESH,
        )

    def advance(self, step):
        if step > 0:
            self.ring_copy(step - 1).wait_recv()
        if step < self.pairs - 1:
            self.ring_copy(step).start()
        self.flip_copy(step).start()
        if self.split and step == self.pairs - 1:
            self.take(step - 1)
            self.rest_copy().start()

    def take(self, step):
        if step in self.taken:
            return
        self.taken.add(step)
        self.flip_copy(step).wait_recv()
        if self.split and step == self.pairs - 1:
            self.rest_copy().wait_recv()

    def finish(self):
        for step in range(self.pairs):
            if step < self.pairs - 1:
                self.ring_copy(step).wait_send()
            self.flip_copy(step).wait_send()
        if self.split:
            self.rest_copy().wait_send()


def gather_sems(n):
    pairs = n // 2
    return [
        pltpu.SemaphoreType.DMA((pairs,)),
        pltpu.SemaphoreType.DMA((pairs,)),
        pltpu.SemaphoreType.DMA((pairs,)),
        pltpu.SemaphoreType.DMA((pairs,)),
    ]


def greet(axes):
    barrier = pltpu.get_barrier_semaphore()
    count = 0
    for axis in axes:
        n = lax.axis_size(axis)
        me = lax.axis_index(axis)
        pl.semaphore_signal(
            barrier, 1, device_id={axis: me + 1 - 2 * lax.rem(me, 2)}, device_id_type=MESH
        )
        for k in range(1, n // 2):
            pl.semaphore_signal(
                barrier, 1, device_id={axis: lax.rem(me + 2 * k, n)}, device_id_type=MESH
            )
        count += n // 2
    pl.semaphore_wait(barrier, count)


def send(src, dst, sems, index, device):
    return pltpu.make_async_remote_copy(
        src_ref=src,
        dst_ref=dst,
        send_sem=sems[0].at[index],
        recv_sem=sems[1].at[index],
        device_id=device,
        device_id_type=MESH,
    )


def server_kernel(
    cut_own, cot_own, attended_own, normed_own, gain, gate_hbm, up_hbm, down_hbm,
    server_out, cut_grad, attended_far, normed_far, rows_normed_far, rows_cot_far,
    hidden_far, d_gate_far, d_up_far,
    attended_all, normed_all, rows_normed, rows_cot, hidden, d_gate, d_up, store_sem,
    gate_w, up_w, down_w, cut_slots, served, served_in, home_in, home_out, sums, give, give_in,
    passing, pass_in, load_sem, cut_sems, cot_sems, attended_sems, normed_sems, swap_sems, part_sems,
    home_sems, pass_sems,
):
    members, groups = lax.axis_size("mem"), lax.axis_size("grp")
    pairs, group_pairs = members // 2, groups // 2
    length, width = cut_own.shape
    half = length // 2
    me = lax.axis_index("mem")
    odd = lax.rem(me, 2)
    partner = {"mem": me + 1 - 2 * odd}
    loads = []
    for i, (far, near) in enumerate(((down_hbm, down_w), (gate_hbm, gate_w), (up_hbm, up_w))):
        loads.append(pltpu.make_async_copy(far, near, load_sem.at[i]))
        loads[-1].start()
    greet(("grp", "mem"))
    cut = Gather("mem", cut_own, cut_slots, cut_sems)
    cot = Gather("mem", cot_own, rows_cot, cot_sems)
    early = [
        Gather("grp", normed_own, normed_all, normed_sems, True),
        Gather("grp", attended_own, attended_all, attended_sems, True),
    ]
    cut.advance(0)
    cot.advance(0)
    for chain in early:
        chain.advance(0)
    cut_slots[0] = cut_own[...]
    rows_cot[0] = cot_own[...]
    normed_all[0] = normed_own[...]
    attended_all[0] = attended_own[...]
    sums[...] = cot_own[...].astype(F32)
    swaps = []
    pending = [(chain, step) for step in range(1, group_pairs) for chain in early]
    stores = []

    def keep_going():
        if pending:
            chain, step = pending.pop(0)
            chain.advance(step)

    def store(near, far):
        stores.append(pltpu.make_async_copy(near, far, store_sem.at[len(stores)]))
        stores[-1].start()

    for p in range(pairs):
        if p > 0:
            cut.advance(p)
            cot.advance(p)
        cut.take(p)
        cot.take(p)
        span = pl.ds(2 * p, 2)
        h_float = cut_slots[span].reshape(2 * length, width).astype(F32)
        inv_rms = rms(h_float)
        normed = (h_float * inv_rms * gain[...]).astype(BF16)
        rows_normed[span] = normed.reshape(2, length, width)
        if p == 0:
            for load in loads:
                load.wait()
        d_hidden = lax.dot_general(
            rows_cot[span].reshape(2 * length, width), down_w[...], CONTRACT_LAST,
            preferred_element_type=F32,
        )
        gate_act = lax.dot_general(normed, gate_w[...], CONTRACT_LAST, preferred_element_type=F32)
        up_act = lax.dot_general(normed, up_w[...], CONTRACT_LAST, preferred_element_type=F32)
        keep_going()
        sigma = jax.nn.sigmoid(gate_act)
        acted = gate_act * sigma
        hidden_now = (acted * up_act).astype(BF16)
        dg = (d_hidden * up_act * sigma * (1.0 + gate_act * (1.0 - sigma))).astype(BF16)
        du = (d_hidden * acted).astype(BF16)
        rows = pl.ds(2 * p * length, 2 * length)
        hidden[rows] = hidden_now
        d_gate[rows] = dg
        d_up[rows] = du
        d_normed = jnp.dot(dg, gate_w[...], preferred_element_type=F32)
        d_normed = d_normed + jnp.dot(du, up_w[...], preferred_element_type=F32)
        pushed = norm_back(h_float, inv_rms, gain[...], d_normed)
        sums[...] += pushed[:length] + pushed[length:]
        served[span] = (
            jnp.dot(hidden_now, down_w[...], preferred_element_type=F32)
            .astype(BF16)
            .reshape(2, length, width)
        )
        keep_going()
        for near, far in (
            (hidden, hidden_far), (d_gate, d_gate_far), (d_up, d_up_far)
        ):
            store(near.at[rows], far.at[rows])
        store(rows_normed.at[span], rows_normed_far.at[span])
        store(rows_cot.at[span], rows_cot_far.at[span])

    keep_rows = pl.ds(pl.multiple_of(odd * half, half), half)
    give_rows = pl.ds(pl.multiple_of((1 - odd) * half, half), half)
    give[...] = sums[give_rows].astype(BF16)
    handed = send(give, give_in, part_sems, 0, partner)
    handed.start()
    for p in range(pairs):
        swaps.append(send(served.at[2 * p + 1], served_in.at[p], swap_sems, p, partner))
        swaps[-1].start()
    handed.wait_recv()
    keep_going()
    total = sums[keep_rows] + give_in[...].astype(F32)
    passing[...] = total.astype(BF16)
    passes = []
    for k in range(1, pairs):
        passes.append(
            send(passing, pass_in.at[k - 1], pass_sems, k - 1, {"mem": lax.rem(me + 2 * k, members)})
        )
        passes[-1].start()
    homes = []
    for p in range(pairs):
        swaps[p].wait_recv()
        mine = served[2 * p].astype(F32) + served_in[p].astype(F32)
        if p == 0:
            result = cut_own[...].astype(F32) + mine
            sums[...] = result
        else:
            home_out[p - 1] = mine.astype(BF16)
            homes.append(
                send(
                    home_out.at[p - 1], home_in.at[p - 1], home_sems, p - 1,
                    {"mem": lax.rem(me + members - 2 * p, members)},
                )
            )
            homes[-1].start()
    for k in range(1, pairs):
        passes[k - 1].wait_recv()
        total = total + pass_in[k - 1].astype(F32)
    cut_grad[keep_rows] = (total / members).astype(BF16)
    back = send(cut_grad.at[keep_rows], cut_grad.at[keep_rows], part_sems, 1, partner)
    back.start()
    result = sums[...]
    for p in range(1, pairs):
        homes[p - 1].wait_recv()
        result = result + home_in[p - 1].astype(F32)
    server_out[...] = result.astype(BF16)
    while pending:
        keep_going()
    for chain, far in zip(early, (normed_far, attended_far)):
        for step in range(group_pairs):
            chain.take(step)
        store(chain.slots, far)
    for chain in early:
        chain.finish()
    for copy in stores:
        copy.wait()
    cut.finish()
    cot.finish()
    back.wait_recv()
    for copy in [handed, back] + swaps + passes + homes:
        copy.wait_send()


def server_call(cut, cot, attended, normed, gain, gate_t, up_t, down):
    members, groups = lax.axis_size("mem"), lax.axis_size("grp")
    pairs = members // 2
    length, width = cut.shape
    units = down.shape[0]
    half = length // 2
    rows = members * length
    shape = jax.ShapeDtypeStruct
    vmem = pl.BlockSpec(memory_space=pltpu.VMEM)
    far = pl.BlockSpec(memory_space=pl.ANY)
    others = max(pairs - 1, 1)
    two = lambda count: [pltpu.SemaphoreType.DMA((count,))] * 2
    return pl.pallas_call(
        server_kernel,
        out_shape=[
            shape((length, width), BF16),
            shape((length, width), BF16),
            shape((groups, length, width), BF16),
            shape((groups, length, width), BF16),
            shape((members, length, width), BF16),
            shape((members, length, width), BF16),
            shape((rows, units), BF16),
            shape((rows, units), BF16),
            shape((rows, units), BF16),
        ],
        in_specs=[vmem] * 5 + [far] * 3,
        out_specs=[vmem] * 2 + [far] * 7,
        scratch_shapes=[
            pltpu.VMEM((groups, length, width), BF16),
            pltpu.VMEM((groups, length, width), BF16),
            pltpu.VMEM((members, length, width), BF16),
            pltpu.VMEM((members, length, width), BF16),
            pltpu.VMEM((rows, units), BF16),
            pltpu.VMEM((rows, units), BF16),
            pltpu.VMEM((rows, units), BF16),
            pltpu.SemaphoreType.DMA((5 * pairs + 2,)),
            pltpu.VMEM((units, width), BF16),
            pltpu.VMEM((units, width), BF16),
            pltpu.VMEM((units, width), BF16),
            pltpu.VMEM((members, length, width), BF16),
            pltpu.VMEM((members, length, width), BF16),
            pltpu.VMEM((pairs, length, width), BF16),
            pltpu.VMEM((others, length, width), BF16),
            pltpu.VMEM((others, length, width), BF16),
            pltpu.VMEM((length, width), F32),
            pltpu.VMEM((half, width), BF16),
            pltpu.VMEM((half, width), BF16),
            pltpu.VMEM((half, width), BF16),
            pltpu.VMEM((others, half, width), BF16),
            pltpu.SemaphoreType.DMA((3,)),
            gather_sems(members),
            gather_sems(members),
            gather_sems(groups),
            gather_sems(groups),
            two(pairs),
            two(2),
            two(others),
            two(others),
        ],
        compiler_params=pltpu.CompilerParams(
            collective_id=0, has_side_effects=True, vmem_limit_bytes=60 * 2**20
        ),
        name="server",
    )(cut, cot, attended, normed, gain, gate_t, up_t, down)


def grads_kernel(
    d_own, cut_own, attended_far, normed_far, rows_normed_far, rows_cot_far,
    hidden_far, d_gate_far, d_up_far,
    grad_query, grad_keyval, grad_out, grad_gate_far, grad_up_far, grad_down_far,
    attended_all, normed_all, rows_normed, rows_cot, hidden, d_gate, d_up,
    grad_gate, grad_up, grad_down,
    d_slots, half_slots, half_in, acc, d_sems, half_sems, swap_sems, load_sem, store_sem,
):
    groups = lax.axis_size("grp")
    group_pairs = groups // 2
    length, width = cut_own.shape
    half = length // 2
    rows = rows_cot.shape[0] * length
    me = lax.axis_index("mem")
    odd = lax.rem(me, 2)
    half_own = cut_own.at[pl.ds(pl.multiple_of(odd * half, half), half)]
    partner = {"mem": me + 1 - 2 * odd}
    loads = []
    for i, (far, near) in enumerate((
        (hidden_far, hidden), (rows_cot_far, rows_cot), (d_gate_far, d_gate),
        (rows_normed_far, rows_normed), (d_up_far, d_up), (normed_far, normed_all),
        (attended_far, attended_all),
    )):
        loads.append(pltpu.make_async_copy(far, near, load_sem.at[i]))
        loads[-1].start()
    greet(("grp", "mem"))
    halves = Gather("grp", half_own, half_slots, half_sems, True)
    deltas = Gather("grp", d_own, d_slots, d_sems, True)
    chains = [halves, deltas]
    for chain in chains:
        chain.advance(0)
    half_slots[0] = half_own[...]
    d_slots[0] = d_own[...]
    pending = [(chain, step) for step in range(1, group_pairs) for chain in chains]

    def keep_going():
        if pending:
            chain, step = pending.pop(0)
            chain.advance(step)

    def weight_grad(left, right, out):
        out[...] = lax.dot_general(
            left[...], right[...].reshape(rows, width), CONTRACT_FIRST, preferred_element_type=F32
        ).astype(BF16)

    for load in loads:
        load.wait()
    stores = []
    for i, (left, right, near, far) in enumerate((
        (hidden, rows_cot, grad_down, grad_down_far),
        (d_gate, rows_normed, grad_gate, grad_gate_far),
        (d_up, rows_normed, grad_up, grad_up_far),
    )):
        weight_grad(left, right, near)
        stores.append(pltpu.make_async_copy(near, far, store_sem.at[i]))
        stores[-1].start()
        keep_going()
    while pending:
        keep_going()

    def grad_in(first, count):
        return lax.dot_general(
            normed_all[pl.ds(first, count)].reshape(count * length, width),
            d_slots[pl.ds(first, count)].reshape(count * length, d_slots.shape[2]),
            CONTRACT_FIRST,
            preferred_element_type=F32,
        )

    scale = 1.0 / groups
    ready = groups - 2
    for step in range(group_pairs - 1):
        deltas.take(step)
    acc[...] = grad_in(0, ready)
    for step in range(group_pairs):
        halves.take(step)
    swap = send(half_slots, half_in, swap_sems, 0, partner)
    swap.start()
    swap.wait_recv()
    mine = half_slots[...]
    other = half_in[...]
    top = jnp.where(odd == 0, mine, other)
    bottom = jnp.where(odd == 0, other, mine)
    top_att = attended_all[:, pl.ds(0, half), :].reshape(groups * half, width)
    low_att = attended_all[:, pl.ds(half, half), :].reshape(groups * half, width)
    out = lax.dot_general(
        top_att, top.reshape(groups * half, width), CONTRACT_FIRST, preferred_element_type=F32
    )
    out = out + lax.dot_general(
        low_att, bottom.reshape(groups * half, width), CONTRACT_FIRST, preferred_element_type=F32
    )
    grad_out[...] = (out * scale).astype(BF16)
    deltas.take(group_pairs - 1)
    split = grad_query.shape[1]
    result = (acc[...] + grad_in(ready, 2)) * scale
    grad_query[...] = result[:, :split].astype(BF16)
    grad_keyval[...] = result[:, split:].astype(BF16)
    for chain in chains:
        chain.finish()
    swap.wait_send()
    for copy in stores:
        copy.wait()


def grads_call(
    columns, d_own, cut_grad, attended_all, normed_all, rows_normed, rows_cot, hidden, d_gate, d_up
):
    groups = lax.axis_size("grp")
    width, (length, wide) = cut_grad.shape[1], d_own.shape
    half = length // 2
    units = hidden.shape[1]
    shape = jax.ShapeDtypeStruct
    vmem = pl.BlockSpec(memory_space=pltpu.VMEM)
    far = pl.BlockSpec(memory_space=pl.ANY)
    wide_operands = [attended_all, normed_all, rows_normed, rows_cot, hidden, d_gate, d_up]
    return pl.pallas_call(
        grads_kernel,
        out_shape=[
            shape((width, columns), BF16),
            shape((width, wide - columns), BF16),
            shape((width, width), BF16),
            shape((units, width), BF16),
            shape((units, width), BF16),
            shape((units, width), BF16),
        ],
        in_specs=[vmem] * 2 + [far] * 7,
        out_specs=[vmem] * 3 + [far] * 3,
        scratch_shapes=[pltpu.VMEM(a.shape, BF16) for a in wide_operands]
        + [pltpu.VMEM((units, width), BF16)] * 3
        + [
            pltpu.VMEM((groups, length, wide), BF16),
            pltpu.VMEM((groups, half, width), BF16),
            pltpu.VMEM((groups, half, width), BF16),
            pltpu.VMEM((width, wide), F32),
            gather_sems(groups),
            gather_sems(groups),
            [pltpu.SemaphoreType.DMA((1,))] * 2,
            pltpu.SemaphoreType.DMA((7,)),
            pltpu.SemaphoreType.DMA((3,)),
        ],
        compiler_params=pltpu.CompilerParams(
            collective_id=1, has_side_effects=True, vmem_limit_bytes=60 * 2**20
        ),
        name="grads",
    )(d_own, cut_grad, *wide_operands)


def hand_over_kernel(count, *refs):
    fars, outs, nears = refs[:count], refs[count : 2 * count], refs[2 * count : 3 * count]
    load_sem, store_sem = refs[3 * count :]
    pieces = []
    for far, out, near in zip(fars, outs, nears):
        rows = far.shape[0]
        parts = 2 if rows % 32 == 0 else 1
        for part in range(parts):
            span = pl.ds(part * (rows // parts), rows // parts)
            i = len(pieces)
            pieces.append((
                pltpu.make_async_copy(far.at[span], near.at[span], load_sem.at[i]),
                pltpu.make_async_copy(near.at[span], out.at[span], store_sem.at[i]),
            ))
    for load, _ in pieces:
        load.start()
    for load, store in pieces:
        load.wait()
        store.start()
    for _, store in pieces:
        store.wait()


def hand_over(arrays):
    far = pl.BlockSpec(memory_space=pl.ANY)
    count = len(arrays)
    return pl.pallas_call(
        functools.partial(hand_over_kernel, count),
        out_shape=[jax.ShapeDtypeStruct(a.shape, a.dtype) for a in arrays],
        in_specs=[far] * count,
        out_specs=[far] * count,
        scratch_shapes=[pltpu.VMEM(a.shape, a.dtype) for a in arrays]
        + [pltpu.SemaphoreType.DMA((2 * count,))] * 2,
        compiler_params=pltpu.CompilerParams(vmem_limit_bytes=60 * 2**20),
        name="results",
    )(*arrays)


def on_device(
    client_input,
    client_gain,
    w_query,
    w_keyval,
    w_out,
    server_gain,
    w_gate,
    w_up,
    w_down,
    out_grad,
    valid,
):
    tokens_in = client_input[0, 0]
    output_w = w_out[0]
    length, width = tokens_in.shape
    live = jnp.arange(length) < valid[0, 0]
    own_cot = jnp.where(live[:, None], out_grad[0, 0], jnp.zeros_like(out_grad[0, 0]))

    x_float = tokens_in.astype(F32)
    client_normed = (x_float * rms(x_float) * client_gain[0]).astype(BF16)
    queries = jnp.dot(client_normed, w_query[0], preferred_element_type=F32).astype(BF16)
    key_vals = jnp.dot(client_normed, w_keyval[0], preferred_element_type=F32).astype(BF16)
    attended, pull = jax.vjp(attention, queries, key_vals)
    mixed = jnp.dot(attended, output_w, preferred_element_type=F32)
    own_cut = (x_float + mixed).astype(BF16)

    (server_out, cut_grad, attended_all, normed_all, *rest) = server_call(
        own_cut, own_cot, attended, client_normed, server_gain, w_gate[0].T, w_up[0].T, w_down[0]
    )

    d_attended = lax.dot_general(
        cut_grad, output_w, CONTRACT_LAST, preferred_element_type=F32
    ).astype(BF16)
    d_queries, d_key_vals = pull(d_attended)
    grad_query, grad_keyval, grad_out, grad_gate, grad_up, grad_down = grads_call(
        queries.shape[1], jnp.concatenate([d_queries, d_key_vals], axis=1), cut_grad, attended_all, normed_all, *rest
    )
    (server_out, grad_query, grad_keyval, grad_out, grad_gate, grad_up, grad_down) = hand_over(
        [server_out, grad_query, grad_keyval, grad_out, grad_gate, grad_up, grad_down]
    )
    return (
        server_out[None, None],
        grad_query[None],
        grad_keyval[None],
        grad_out[None],
        grad_gate.T[None],
        grad_up.T[None],
        grad_down[None],
    )


def solution(mesh):
    in_specs = (
        P("grp", "mem", None, None),
        P("mem", None),
        P("mem", None, None),
        P("mem", None, None),
        P("mem", None, None),
        P("grp", None),
        P("grp", None, "mem"),
        P("grp", None, "mem"),
        P("grp", "mem", None),
        P("grp", "mem", None, None),
        P("grp", "mem"),
    )
    out_specs = (
        P("grp", "mem", None, None),
        P("mem", None, None),
        P("mem", None, None),
        P("mem", None, None),
        P("grp", None, "mem"),
        P("grp", None, "mem"),
        P("grp", "mem", None),
    )
    return jax.shard_map(
        on_device, mesh=mesh, in_specs=in_specs, out_specs=out_specs, check_vma=False
    )
```
